128 devices in a mesh: gx: 8 (over z, core), gy: 2 (over x_lo), gz: 8 (over y, x_hi).
Axes of the slice: x: 4 (x_hi: 2, x_lo: 2; x = x_hi * 2 + x_lo), y: 4, z: 4, core: 2. Of those that a mesh axis runs over, the one named last changes fastest.
Arguments:
- amplitudes: float32 [2, 33554432], P(None, ('gx', 'gy', 'gz')), may hold values from -6 to 6
- couplings: float32 [25], replicated, may hold values from -1.2 to 1.2
- fields: float32 [25], replicated, may hold values from 0.3 to 1.2
Outputs:
- evolved: float32 [2, 33554432], P(None, ('gx', 'gy', 'gz'))
The draws below stay inside these ranges and needn't reach their ends.
All inputs are finite; a program needn't handle non-finite values.
Results may differ from the reference program's by a relative error of at most 0.000098.
Values sent between devices are 32-bit elements; how exact they have to be, the bound alone decides.
No kernel may reach another device: no remote copies, remote signals or barrier semaphores. Data moves between devices by JAX's collectives and lax.ppermute only.
A program may use at most 64 MiB of HBM per device.

```python
import jax
import jax.numpy as jnp

NQ = 25
NAMP = 33554432


def levels(rng, shape, shards, least, high):
    factor_of, own = 1.0, jax.random.fold_in(rng, 6)
    for axis_at, parts in shards:
        heights = jnp.exp(jax.random.uniform(jax.random.fold_in(own, axis_at), (parts,), jnp.float32, least / len(shards), high / len(shards)))
        factor_of = factor_of * jnp.repeat(heights, shape[axis_at] // parts).reshape([-1 if axis == axis_at else 1 for axis in range(len(shape))])
    return factor_of


def normal_values(own_key, shape, width, most, shards=(), held_as=jnp.bfloat16):
    level = levels(own_key, shape, shards, -0.22, 0.18) if shards else 1.0
    entries = jax.random.normal(own_key, shape, jnp.float32) * width * level
    return jnp.minimum(jnp.maximum(entries, -most), most).astype(held_as)


def setup_inputs(seed: int = 0) -> dict:
    arg_keys = jax.random.split(jax.random.key(seed), 4)
    amplitudes = normal_values(arg_keys[0], (2, NAMP), 1.0, 6.0, ((1, 128),), jnp.float32)
    couplings = jnp.clip(jax.random.uniform(arg_keys[1], (NQ,), jnp.float32, -1.2, 1.2), -1.2, 1.2)
    fields = jnp.clip(jax.random.uniform(arg_keys[2], (NQ,), jnp.float32, 0.3, 1.2), 0.3, 1.2)
    return {"amplitudes": amplitudes, "couplings": couplings, "fields": fields}


def zz_phases(amplitudes, couplings):
    length_all = amplitudes.shape[1]
    qubits = couplings.shape[0]
    positions = jnp.arange(length_all, dtype=jnp.int32)
    phases = jnp.zeros((length_all,), jnp.float32)
    for bond_index in range(qubits):
        follow = (bond_index + 1) % qubits
        parity = ((positions >> bond_index) ^ (positions >> follow)) & 1
        phases = phases + couplings[bond_index] * (1.0 - 2.0 * parity.astype(jnp.float32))
    cos_phase = jnp.cos(phases)
    sin_phase = jnp.sin(phases)
    real_part = amplitudes[0] * cos_phase + amplitudes[1] * sin_phase
    imag_part = amplitudes[1] * cos_phase - amplitudes[0] * sin_phase
    return real_part, imag_part


def rotate_all(real_part, imag_part, fields):
    length_all = real_part.shape[0]
    for qubit_index in range(fields.shape[0]):
        cosine = jnp.cos(fields[qubit_index])
        sine_value = jnp.sin(fields[qubit_index])
        shape_now = (length_all >> (qubit_index + 1), 2, 1 << qubit_index)
        shaped_real = real_part.reshape(shape_now)
        shaped_imag = imag_part.reshape(shape_now)
        lower_real = shaped_real[:, 0]
        upper_real = shaped_real[:, 1]
        lower_imag = shaped_imag[:, 0]
        upper_imag = shaped_imag[:, 1]
        new_lower_real = cosine * lower_real + sine_value * upper_imag
        new_lower_imag = cosine * lower_imag - sine_value * upper_real
        new_upper_real = cosine * upper_real + sine_value * lower_imag
        new_upper_imag = cosine * upper_imag - sine_value * lower_real
        real_part = jnp.stack([new_lower_real, new_upper_real], axis=1).reshape(length_all)
        imag_part = jnp.stack([new_lower_imag, new_upper_imag], axis=1).reshape(length_all)
    return real_part, imag_part


def reference(amplitudes, couplings, fields):
    real_part, imag_part = zz_phases(amplitudes, couplings)
    real_part, imag_part = rotate_all(real_part, imag_part, fields)
    return jnp.stack([real_part, imag_part])
```

```python
import jax
import jax.numpy as jnp
from jax import lax
from jax.experimental import pallas as pl
from jax.experimental.pallas import tpu as pltpu
from jax.sharding import PartitionSpec as P


AXES = ("gx", "gy", "gz")
SIZES = (688, 688, 680, 680, 680, 680)
STARTS = tuple(sum(SIZES[:i]) for i in range(len(SIZES)))
F32 = jnp.float32
BF16 = jnp.bfloat16


def pair_table():
    place, table = {}, {}
    for gx in range(8):
        for gy in range(2):
            for gz in range(8):
                place[(gx >> 1, gx & 1, (gz & 1) * 2 + gy, gz >> 1)] = (gx * 2 + gy) * 8 + gz
    for (z, core, x, y), device in place.items():
        table[device] = {
            "core": core,
            "c": place[(z, core ^ 1, x, y)],
            "xA": place[(z, core, x ^ 1, y)],
            "xB": place[(z, core, x ^ 3, y)],
            "yA": place[(z, core, x, y ^ 1)],
            "yB": place[(z, core, x, y ^ 3)],
            "zA": place[(z ^ 1, core, x, y)],
            "zB": place[(z ^ 3, core, x, y)],
        }
    return table


def pairs_of(dim, first):
    table = pair_table()
    if dim == "c":
        return [(d, row["c"]) for d, row in table.items()]
    return [(d, row[dim + ("A" if (row["core"] == 0) == first else "B")]) for d, row in table.items()]


def spin(value, bit):
    return 1.0 - 2.0 * ((value >> bit) & 1).astype(F32)


def ones_in(value, bits):
    total = value & 1
    for bit in range(1, bits):
        total = total + ((value >> bit) & 1)
    return total


def turn(cosine, sine, quarter):
    quarter = quarter & 3
    odd = (quarter & 1) == 1
    real = jnp.where(odd, sine, cosine)
    imag = jnp.where(odd, cosine, -sine)
    sign = jnp.where(quarter >= 2, -1.0, 1.0)
    return real * sign, imag * sign


def split(value):
    high = value.astype(BF16)
    return high, (value - high.astype(F32)).astype(BF16)


def rotation(tangents, first, right):
    rows = lax.broadcasted_iota(jnp.int32, (128, 128), 0)
    cols = lax.broadcasted_iota(jnp.int32, (128, 128), 1)
    out_at, in_at = (cols, rows) if right else (rows, cols)
    differ = out_at ^ in_at
    result = jnp.ones((128, 128), F32)
    for bit in range(7):
        tangent = tangents[first + bit : first + bit + 1, :]
        signed = jnp.where(((out_at >> bit) & 1) == 1, tangent, -tangent)
        result = result * jnp.where(((differ >> bit) & 1) == 1, signed, 1.0)
    return result


def device_bits():
    number = (lax.axis_index("gx") * 2 + lax.axis_index("gy")) * 8 + lax.axis_index("gz")
    return number


def local_kernel(x_ref, j_ref, f_ref, *refs):
    outs, coef_ref, z_ref = refs[: len(SIZES)], refs[len(SIZES)], refs[len(SIZES) + 1]
    number = device_bits()
    bits = [(number >> k) & 1 for k in range(7)]
    sigma = [1.0 - 2.0 * b.astype(F32) for b in bits]
    row_at = lax.broadcasted_iota(jnp.int32, (32, 128), 0)
    angles = jnp.zeros((32, 128), F32)
    for q in range(25):
        angles = jnp.where(row_at == q, f_ref[q], angles)
    cosines = jnp.cos(angles)
    tangents = jnp.sin(angles) / cosines
    scale = cosines[0:1, :]
    for q in range(1, 25):
        scale = scale * cosines[q : q + 1, :]

    on_core0 = bits[4] == 0
    table = jnp.zeros((16, 128), F32)
    row16 = lax.broadcasted_iota(jnp.int32, (16, 128), 0)

    def put(table, row, value):
        return jnp.where(row16 == row, value, table)

    for k, (q0, q1) in enumerate(((21, 18), (19, 20), (23, 24))):
        s0 = -sigma[q0 - 18] * tangents[q0 : q0 + 1, :]
        s1 = -sigma[q1 - 18] * tangents[q1 : q1 + 1, :]
        both = s0 * s1
        table = put(table, 3 * k, jnp.where(on_core0, s0, both))
        table = put(table, 3 * k + 1, jnp.where(on_core0, both, -s0))
        table = put(table, 3 * k + 2, jnp.where(on_core0, -s1, s1))
    table = put(table, 9, -sigma[4] * tangents[22:23, :])
    coef_ref[...] = table

    low = lax.broadcasted_iota(jnp.int32, (16, 128), 0) * 128 + lax.broadcasted_iota(jnp.int32, (16, 128), 1)
    spins = [spin(low, q) for q in range(11)]
    phase = j_ref[24] * sigma[6] * spins[0]
    for q in range(10):
        phase = phase + j_ref[q] * (spins[q] * spins[q + 1])
    e1r, e1i = turn(jnp.cos(phase), jnp.sin(phase), ones_in(low, 11))
    high = lax.broadcasted_iota(jnp.int32, (8, 128), 1)
    spins = [spin(high, k) for k in range(7)]
    below = spin(lax.broadcasted_iota(jnp.int32, (8, 128), 0), 0)
    phase = j_ref[10] * (below * spins[0]) + (j_ref[17] * sigma[0]) * spins[6]
    for k in range(6):
        phase = phase + j_ref[11 + k] * (spins[k] * spins[k + 1])
    of_device = j_ref[18] * (sigma[0] * sigma[1])
    for k in range(1, 6):
        of_device = of_device + j_ref[18 + k] * (sigma[k] * sigma[k + 1])
    phase = phase + of_device
    device_ones = bits[0] + bits[1] + bits[2] + bits[3] + bits[4] + bits[5] + bits[6]
    e2r, e2i = turn(jnp.cos(phase), jnp.sin(phase), ones_in(high, 7) + device_ones)
    e2r, e2i = e2r * scale, e2i * scale

    lane_hi, lane_lo = split(rotation(tangents, 0, True))
    lane_mat = jnp.concatenate(
        [
            jnp.concatenate([lane_hi, lane_lo], axis=1),
            jnp.concatenate([lane_hi, jnp.zeros((128, 128), BF16)], axis=1),
        ],
        axis=0,
    )
    row_rot = rotation(tangents, 11, False)
    row_mats = []
    for v in range(2):
        mr, mi = row_rot * e2r[v : v + 1, :], row_rot * e2i[v : v + 1, :]
        row_mats.append(
            split(
                jnp.concatenate(
                    [jnp.concatenate([mr, -mi], axis=1), jnp.concatenate([mi, mr], axis=1)], axis=0
                )
            )
        )

    def lanes_done(rl):
        xre = x_ref[pl.ds(2 * rl, 128, stride=32), :]
        xim = x_ref[pl.ds(2 * rl + 1, 128, stride=32), :]
        er, ei = e1r[rl : rl + 1, :], e1i[rl : rl + 1, :]
        y = jnp.concatenate([xre * er - xim * ei, xre * ei + xim * er], axis=0)
        y_hi, y_lo = split(y)
        p = jnp.dot(jnp.concatenate([y_hi, y_lo], axis=1), lane_mat, preferred_element_type=F32)
        return p[:, :128] + p[:, 128:]

    for rl in range(0, 16, 2):
        m_hi, m_lo = row_mats[rl >> 3]
        y_hi, y_lo = split(jnp.concatenate([lanes_done(rl), lanes_done(rl + 1)], axis=1))
        z = jnp.dot(m_hi, y_hi, preferred_element_type=F32)
        z = z + jnp.dot(m_lo, y_hi, preferred_element_type=F32)
        z = z + jnp.dot(m_hi, y_lo, preferred_element_type=F32)
        z_ref[rl] = z[:, :128]
        z_ref[rl + 1] = z[:, 128:]

    low_tangents = [jnp.broadcast_to(tangents[7 + k : 8 + k, :], (8, 128)) for k in range(4)]
    for at in range(0, 256, 8):
        v = [z_ref[rl, at : at + 8, :] for rl in range(16)]
        for k in range(4):
            t = low_tangents[k]
            w = list(v)
            for rl in range(16):
                if rl >> k & 1:
                    w[rl] = v[rl] + t * v[rl ^ (1 << k)]
                else:
                    w[rl] = v[rl] - t * v[rl ^ (1 << k)]
            v = w
        for rl in range(16):
            row = rl * 256 + at
            s = max(i for i in range(len(SIZES)) if STARTS[i] <= row)
            outs[s][row - STARTS[s] : row - STARTS[s] + 8, :] = v[rl]


def final_kernel(*refs):
    ins, out_ref = refs[: len(SIZES)], refs[len(SIZES)]
    number = device_bits()
    device_ones = number & 1
    for k in range(1, 7):
        device_ones = device_ones + ((number >> k) & 1)
    rows = lax.broadcasted_iota(jnp.int32, (128, 128), 0)
    cols = lax.broadcasted_iota(jnp.int32, (128, 128), 1)
    base = ones_in(rows, 7) + ones_in(cols, 7) + device_ones

    def read(start):
        parts = []
        row = start
        while row < start + 128:
            s = max(i for i in range(len(SIZES)) if STARTS[i] <= row)
            stop = min(start + 128, STARTS[s] + SIZES[s])
            parts.append(ins[s][row - STARTS[s] : stop - STARTS[s], :])
            row = stop
        return parts[0] if len(parts) == 1 else jnp.concatenate(parts, axis=0)

    for rl in range(16):
        re, im = read(rl * 256), read(rl * 256 + 128)
        quarter = (base + bin(rl).count("1")) & 3
        odd = (quarter & 1) == 1
        out_re = jnp.where(odd, im, re)
        out_im = jnp.where(odd, re, im)
        out_ref[pl.ds(2 * rl, 128, stride=32), :] = jnp.where(quarter >= 2, -out_re, out_re)
        out_ref[pl.ds(2 * rl + 1, 128, stride=32), :] = jnp.where(
            (quarter == 1) | (quarter == 2), -out_im, out_im
        )


def shards(amplitudes, couplings, fields):
    rows = amplitudes.reshape(2, 2048, 128).transpose(1, 0, 2).reshape(4096, 128)
    vmem = pl.BlockSpec(memory_space=pltpu.VMEM)
    smem = pl.BlockSpec(memory_space=pltpu.SMEM)
    made = pl.pallas_call(
        local_kernel,
        out_shape=[jax.ShapeDtypeStruct((s, 128), F32) for s in SIZES] + [jax.ShapeDtypeStruct((16, 128), F32)],
        in_specs=[vmem, smem, smem],
        out_specs=[vmem] * (len(SIZES) + 1),
        scratch_shapes=[pltpu.VMEM((16, 256, 128), F32)],
        name="local_step",
    )(rows, couplings, fields)
    streams, coef = list(made[:-1]), made[-1]

    def swap_core(value):
        return value + coef[9:10] * lax.ppermute(value, AXES, pairs_of("c", True))

    count = len(streams)
    for i in range(count // 2, count):
        streams[i] = swap_core(streams[i])
    kept = [None] * count
    for step in range(6):
        first = step % 2 == 0
        for i in range(count):
            k = (step // 2 + i) % 3
            got = lax.ppermute(streams[i], AXES, pairs_of("xyz"[k], first))
            if first:
                mine = streams[i]
                kept[i] = mine + coef[3 * k : 3 * k + 1] * got
                streams[i] = coef[3 * k + 1 : 3 * k + 2] * mine + coef[3 * k + 2 : 3 * k + 3] * got
            else:
                streams[i] = kept[i] + got
    for i in range(count // 2):
        streams[i] = swap_core(streams[i])
    out = pl.pallas_call(
        final_kernel,
        out_shape=jax.ShapeDtypeStruct((4096, 128), F32),
        in_specs=[vmem] * count,
        out_specs=vmem,
        name="final_step",
    )(*streams)
    return out.reshape(2048, 2, 128).transpose(1, 0, 2).reshape(2, 262144)


def solution(mesh):
    placed = (P(None, AXES), P(), P())
    return jax.shard_map(shards, mesh=mesh, in_specs=placed, out_specs=P(None, AXES), check_vma=False)
```

```python
import jax
import jax.numpy as jnp
from jax import lax
from jax.experimental import pallas as pl
from jax.experimental.pallas import tpu as pltpu
from jax.sharding import PartitionSpec as P


AXES = ("gx", "gy", "gz")
SIZES = (656, 672, 680, 688, 696, 704)
STARTS = tuple(sum(SIZES[:i]) for i in range(len(SIZES)))
F32 = jnp.float32
BF16 = jnp.bfloat16


def pair_table():
    place, table = {}, {}
    for gx in range(8):
        for gy in range(2):
            for gz in range(8):
                place[(gx >> 1, gx & 1, (gz & 1) * 2 + gy, gz >> 1)] = (gx * 2 + gy) * 8 + gz
    for (z, core, x, y), device in place.items():
        table[device] = {
            "core": core,
            "c": place[(z, core ^ 1, x, y)],
            "xA": place[(z, core, x ^ 1, y)],
            "xB": place[(z, core, x ^ 3, y)],
            "yA": place[(z, core, x, y ^ 1)],
            "yB": place[(z, core, x, y ^ 3)],
            "zA": place[(z ^ 1, core, x, y)],
            "zB": place[(z ^ 3, core, x, y)],
        }
    return table


def pairs_of(dim, first):
    table = pair_table()
    if dim == "c":
        return [(d, row["c"]) for d, row in table.items()]
    return [(d, row[dim + ("A" if (row["core"] == 0) == first else "B")]) for d, row in table.items()]


def spin(value, bit):
    return 1.0 - 2.0 * ((value >> bit) & 1).astype(F32)


def ones_in(value, bits):
    total = value & 1
    for bit in range(1, bits):
        total = total + ((value >> bit) & 1)
    return total


def turn(cosine, sine, quarter):
    quarter = quarter & 3
    odd = (quarter & 1) == 1
    real = jnp.where(odd, sine, cosine)
    imag = jnp.where(odd, cosine, -sine)
    sign = jnp.where(quarter >= 2, -1.0, 1.0)
    return real * sign, imag * sign


def split(value):
    high = value.astype(BF16)
    return high, (value - high.astype(F32)).astype(BF16)


def rotation(tangents, first, right):
    rows = lax.broadcasted_iota(jnp.int32, (128, 128), 0)
    cols = lax.broadcasted_iota(jnp.int32, (128, 128), 1)
    out_at, in_at = (cols, rows) if right else (rows, cols)
    differ = out_at ^ in_at
    result = jnp.ones((128, 128), F32)
    for bit in range(7):
        tangent = tangents[first + bit : first + bit + 1, :]
        signed = jnp.where(((out_at >> bit) & 1) == 1, tangent, -tangent)
        result = result * jnp.where(((differ >> bit) & 1) == 1, signed, 1.0)
    return result


def device_bits():
    number = (lax.axis_index("gx") * 2 + lax.axis_index("gy")) * 8 + lax.axis_index("gz")
    return number


def local_kernel(x_ref, j_ref, f_ref, *refs):
    outs, coef_ref, z_ref = refs[: len(SIZES)], refs[len(SIZES)], refs[len(SIZES) + 1]
    number = device_bits()
    bits = [(number >> k) & 1 for k in range(7)]
    sigma = [1.0 - 2.0 * b.astype(F32) for b in bits]
    row_at = lax.broadcasted_iota(jnp.int32, (32, 128), 0)
    angles = jnp.zeros((32, 128), F32)
    for q in range(25):
        angles = jnp.where(row_at == q, f_ref[q], angles)
    cosines = jnp.cos(angles)
    tangents = jnp.sin(angles) / cosines
    scale = cosines[0:1, :]
    for q in range(1, 25):
        scale = scale * cosines[q : q + 1, :]

    on_core0 = bits[4] == 0
    table = jnp.zeros((16, 128), F32)
    row16 = lax.broadcasted_iota(jnp.int32, (16, 128), 0)

    def put(table, row, value):
        return jnp.where(row16 == row, value, table)

    for k, (q0, q1) in enumerate(((21, 18), (19, 20), (23, 24))):
        s0 = -sigma[q0 - 18] * tangents[q0 : q0 + 1, :]
        s1 = -sigma[q1 - 18] * tangents[q1 : q1 + 1, :]
        both = s0 * s1
        table = put(table, 3 * k, jnp.where(on_core0, s0, both))
        table = put(table, 3 * k + 1, jnp.where(on_core0, both, -s0))
        table = put(table, 3 * k + 2, jnp.where(on_core0, -s1, s1))
    table = put(table, 9, -sigma[4] * tangents[22:23, :])
    coef_ref[...] = table

    low = lax.broadcasted_iota(jnp.int32, (16, 128), 0) * 128 + lax.broadcasted_iota(jnp.int32, (16, 128), 1)
    spins = [spin(low, q) for q in range(11)]
    phase = j_ref[24] * sigma[6] * spins[0]
    for q in range(10):
        phase = phase + j_ref[q] * (spins[q] * spins[q + 1])
    e1r, e1i = turn(jnp.cos(phase), jnp.sin(phase), ones_in(low, 11))
    high = lax.broadcasted_iota(jnp.int32, (8, 128), 1)
    spins = [spin(high, k) for k in range(7)]
    below = spin(lax.broadcasted_iota(jnp.int32, (8, 128), 0), 0)
    phase = j_ref[10] * (below * spins[0]) + (j_ref[17] * sigma[0]) * spins[6]
    for k in range(6):
        phase = phase + j_ref[11 + k] * (spins[k] * spins[k + 1])
    of_device = j_ref[18] * (sigma[0] * sigma[1])
    for k in range(1, 6):
        of_device = of_device + j_ref[18 + k] * (sigma[k] * sigma[k + 1])
    phase = phase + of_device
    device_ones = bits[0] + bits[1] + bits[2] + bits[3] + bits[4] + bits[5] + bits[6]
    e2r, e2i = turn(jnp.cos(phase), jnp.sin(phase), ones_in(high, 7) + device_ones)
    e2r, e2i = e2r * scale, e2i * scale

    lane_hi, lane_lo = split(rotation(tangents, 0, True))
    lane_mat = jnp.concatenate(
        [
            jnp.concatenate([lane_hi, lane_lo], axis=1),
            jnp.concatenate([lane_hi, jnp.zeros((128, 128), BF16)], axis=1),
        ],
        axis=0,
    )
    row_rot = rotation(tangents, 11, False)
    row_mats = []
    for v in range(2):
        mr, mi = row_rot * e2r[v : v + 1, :], row_rot * e2i[v : v + 1, :]
        row_mats.append(
            split(
                jnp.concatenate(
                    [jnp.concatenate([mr, -mi], axis=1), jnp.concatenate([mi, mr], axis=1)], axis=0
                )
            )
        )

    def lanes_done(rl):
        xre = x_ref[pl.ds(2 * rl, 128, stride=32), :]
        xim = x_ref[pl.ds(2 * rl + 1, 128, stride=32), :]
        er, ei = e1r[rl : rl + 1, :], e1i[rl : rl + 1, :]
        y = jnp.concatenate([xre * er - xim * ei, xre * ei + xim * er], axis=0)
        y_hi, y_lo = split(y)
        p = jnp.dot(jnp.concatenate([y_hi, y_lo], axis=1), lane_mat, preferred_element_type=F32)
        return p[:, :128] + p[:, 128:]

    for rl in range(0, 16, 2):
        m_hi, m_lo = row_mats[rl >> 3]
        y_hi, y_lo = split(jnp.concatenate([lanes_done(rl), lanes_done(rl + 1)], axis=1))
        z = jnp.dot(m_hi, y_hi, preferred_element_type=F32)
        z = z + jnp.dot(m_lo, y_hi, preferred_element_type=F32)
        z = z + jnp.dot(m_hi, y_lo, preferred_element_type=F32)
        z_ref[rl] = z[:, :128]
        z_ref[rl + 1] = z[:, 128:]

    low_tangents = [jnp.broadcast_to(tangents[7 + k : 8 + k, :], (8, 128)) for k in range(4)]
    for at in range(0, 256, 8):
        v = [z_ref[rl, at : at + 8, :] for rl in range(16)]
        for k in range(4):
            t = low_tangents[k]
            w = list(v)
            for rl in range(16):
                if rl >> k & 1:
                    w[rl] = v[rl] + t * v[rl ^ (1 << k)]
                else:
                    w[rl] = v[rl] - t * v[rl ^ (1 << k)]
            v = w
        for rl in range(16):
            row = rl * 256 + at
            s = max(i for i in range(len(SIZES)) if STARTS[i] <= row)
            outs[s][row - STARTS[s] : row - STARTS[s] + 8, :] = v[rl]


def final_kernel(*refs):
    ins, out_ref = refs[: len(SIZES)], refs[len(SIZES)]
    number = device_bits()
    device_ones = number & 1
    for k in range(1, 7):
        device_ones = device_ones + ((number >> k) & 1)
    rows = lax.broadcasted_iota(jnp.int32, (128, 128), 0)
    cols = lax.broadcasted_iota(jnp.int32, (128, 128), 1)
    base = ones_in(rows, 7) + ones_in(cols, 7) + device_ones

    def read(start):
        parts = []
        row = start
        while row < start + 128:
            s = max(i for i in range(len(SIZES)) if STARTS[i] <= row)
            stop = min(start + 128, STARTS[s] + SIZES[s])
            parts.append(ins[s][row - STARTS[s] : stop - STARTS[s], :])
            row = stop
        return parts[0] if len(parts) == 1 else jnp.concatenate(parts, axis=0)

    for rl in range(16):
        re, im = read(rl * 256), read(rl * 256 + 128)
        quarter = (base + bin(rl).count("1")) & 3
        odd = (quarter & 1) == 1
        out_re = jnp.where(odd, im, re)
        out_im = jnp.where(odd, re, im)
        out_ref[pl.ds(2 * rl, 128, stride=32), :] = jnp.where(quarter >= 2, -out_re, out_re)
        out_ref[pl.ds(2 * rl + 1, 128, stride=32), :] = jnp.where(
            (quarter == 1) | (quarter == 2), -out_im, out_im
        )


def exchange_order():
    count = len(SIZES)
    half = count // 2
    order = [(i, 0) for i in range(half)] + [(i, "c") for i in range(half, count)] + [(i, 0) for i in range(half, count)]
    for step in range(1, 6):
        order += [(i, step) for i in range(count)]
    return order + [(i, "c") for i in range(half)]


def shards(amplitudes, couplings, fields):
    rows = amplitudes.reshape(2, 2048, 128).transpose(1, 0, 2).reshape(4096, 128)
    vmem = pl.BlockSpec(memory_space=pltpu.VMEM)
    smem = pl.BlockSpec(memory_space=pltpu.SMEM)
    made = pl.pallas_call(
        local_kernel,
        out_shape=[jax.ShapeDtypeStruct((s, 128), F32) for s in SIZES] + [jax.ShapeDtypeStruct((16, 128), F32)],
        in_specs=[vmem, smem, smem],
        out_specs=[vmem] * (len(SIZES) + 1),
        scratch_shapes=[pltpu.VMEM((16, 256, 128), F32)],
        name="local_step",
    )(rows, couplings, fields)
    streams, coef = list(made[:-1]), made[-1]

    count = len(streams)
    kept = [None] * count
    for i, step in exchange_order():
        if step == "c":
            got = lax.ppermute(streams[i], AXES, pairs_of("c", True))
            streams[i] = streams[i] + coef[9:10] * got
            continue
        first = step % 2 == 0
        k = (step // 2 + i) % 3
        got = lax.ppermute(streams[i], AXES, pairs_of("xyz"[k], first))
        if first:
            mine = streams[i]
            kept[i] = mine + coef[3 * k : 3 * k + 1] * got
            streams[i] = coef[3 * k + 1 : 3 * k + 2] * mine + coef[3 * k + 2 : 3 * k + 3] * got
        else:
            streams[i] = kept[i] + got
    out = pl.pallas_call(
        final_kernel,
        out_shape=jax.ShapeDtypeStruct((4096, 128), F32),
        in_specs=[vmem] * count,
        out_specs=vmem,
        name="final_step",
    )(*streams)
    return out.reshape(2048, 2, 128).transpose(1, 0, 2).reshape(2, 262144)


def solution(mesh):
    placed = (P(None, AXES), P(), P())
    return jax.shard_map(shards, mesh=mesh, in_specs=placed, out_specs=P(None, AXES), check_vma=False)
```

```python
import jax
import jax.numpy as jnp
from jax import lax
from jax.experimental import pallas as pl
from jax.experimental.pallas import tpu as pltpu
from jax.sharding import PartitionSpec as P


AXES = ("gx", "gy", "gz")
SIZES = (656, 672, 680, 688, 696, 704)
STARTS = tuple(sum(SIZES[:i]) for i in range(len(SIZES)))
F32 = jnp.float32
BF16 = jnp.bfloat16


def pair_table():
    place, table = {}, {}
    for gx in range(8):
        for gy in range(2):
            for gz in range(8):
                place[(gx >> 1, gx & 1, (gz & 1) * 2 + gy, gz >> 1)] = (gx * 2 + gy) * 8 + gz
    for (z, core, x, y), device in place.items():
        table[device] = {
            "core": core,
            "c": place[(z, core ^ 1, x, y)],
            "xA": place[(z, core, x ^ 1, y)],
            "xB": place[(z, core, x ^ 3, y)],
            "yA": place[(z, core, x, y ^ 1)],
            "yB": place[(z, core, x, y ^ 3)],
            "zA": place[(z ^ 1, core, x, y)],
            "zB": place[(z ^ 3, core, x, y)],
        }
    return table


def pairs_of(dim, first):
    table = pair_table()
    if dim == "c":
        return [(d, row["c"]) for d, row in table.items()]
    return [(d, row[dim + ("A" if (row["core"] == 0) == first else "B")]) for d, row in table.items()]


def spin(value, bit):
    return 1.0 - 2.0 * ((value >> bit) & 1).astype(F32)


def ones_in(value, bits):
    total = value & 1
    for bit in range(1, bits):
        total = total + ((value >> bit) & 1)
    return total


def turn(cosine, sine, quarter):
    quarter = quarter & 3
    odd = (quarter & 1) == 1
    real = jnp.where(odd, sine, cosine)
    imag = jnp.where(odd, cosine, -sine)
    sign = jnp.where(quarter >= 2, -1.0, 1.0)
    return real * sign, imag * sign


def split(value):
    high = value.astype(BF16)
    return high, (value - high.astype(F32)).astype(BF16)


def rotation(tangents, first, right):
    rows = lax.broadcasted_iota(jnp.int32, (128, 128), 0)
    cols = lax.broadcasted_iota(jnp.int32, (128, 128), 1)
    out_at, in_at = (cols, rows) if right else (rows, cols)
    differ = out_at ^ in_at
    result = jnp.ones((128, 128), F32)
    for bit in range(7):
        tangent = tangents[first + bit : first + bit + 1, :]
        signed = jnp.where(((out_at >> bit) & 1) == 1, tangent, -tangent)
        result = result * jnp.where(((differ >> bit) & 1) == 1, signed, 1.0)
    return result


def device_bits():
    number = (lax.axis_index("gx") * 2 + lax.axis_index("gy")) * 8 + lax.axis_index("gz")
    return number


def local_kernel(x_ref, j_ref, f_ref, *refs):
    outs, coef_ref, z_ref = refs[: len(SIZES)], refs[len(SIZES)], refs[len(SIZES) + 1]
    number = device_bits()
    bits = [(number >> k) & 1 for k in range(7)]
    sigma = [1.0 - 2.0 * b.astype(F32) for b in bits]
    row_at = lax.broadcasted_iota(jnp.int32, (32, 128), 0)
    angles = jnp.zeros((32, 128), F32)
    for q in range(25):
        angles = jnp.where(row_at == q, f_ref[q], angles)
    cosines = jnp.cos(angles)
    tangents = jnp.sin(angles) / cosines
    scale = cosines[0:1, :]
    for q in range(1, 25):
        scale = scale * cosines[q : q + 1, :]

    on_core0 = bits[4] == 0
    table = jnp.zeros((16, 128), F32)
    row16 = lax.broadcasted_iota(jnp.int32, (16, 128), 0)

    def put(table, row, value):
        return jnp.where(row16 == row, value, table)

    for k, (q0, q1) in enumerate(((21, 18), (19, 20), (23, 24))):
        s0 = -sigma[q0 - 18] * tangents[q0 : q0 + 1, :]
        s1 = -sigma[q1 - 18] * tangents[q1 : q1 + 1, :]
        both = s0 * s1
        table = put(table, 3 * k, jnp.where(on_core0, s0, both))
        table = put(table, 3 * k + 1, jnp.where(on_core0, both, -s0))
        table = put(table, 3 * k + 2, jnp.where(on_core0, -s1, s1))
    table = put(table, 9, -sigma[4] * tangents[22:23, :])
    coef_ref[...] = table

    low = lax.broadcasted_iota(jnp.int32, (16, 128), 0) * 128 + lax.broadcasted_iota(jnp.int32, (16, 128), 1)
    spins = [spin(low, q) for q in range(11)]
    phase = j_ref[24] * sigma[6] * spins[0]
    for q in range(10):
        phase = phase + j_ref[q] * (spins[q] * spins[q + 1])
    e1r, e1i = turn(jnp.cos(phase), jnp.sin(phase), ones_in(low, 11))
    high = lax.broadcasted_iota(jnp.int32, (8, 128), 1)
    spins = [spin(high, k) for k in range(7)]
    below = spin(lax.broadcasted_iota(jnp.int32, (8, 128), 0), 0)
    phase = j_ref[10] * (below * spins[0]) + (j_ref[17] * sigma[0]) * spins[6]
    for k in range(6):
        phase = phase + j_ref[11 + k] * (spins[k] * spins[k + 1])
    of_device = j_ref[18] * (sigma[0] * sigma[1])
    for k in range(1, 6):
        of_device = of_device + j_ref[18 + k] * (sigma[k] * sigma[k + 1])
    phase = phase + of_device
    device_ones = bits[0] + bits[1] + bits[2] + bits[3] + bits[4] + bits[5] + bits[6]
    e2r, e2i = turn(jnp.cos(phase), jnp.sin(phase), ones_in(high, 7) + device_ones)
    e2r, e2i = e2r * scale, e2i * scale

    lane_hi, lane_lo = split(rotation(tangents, 0, True))
    lane_mat = jnp.concatenate(
        [
            jnp.concatenate([lane_hi, lane_lo], axis=1),
            jnp.concatenate([lane_hi, jnp.zeros((128, 128), BF16)], axis=1),
        ],
        axis=0,
    )
    row_rot = rotation(tangents, 11, False)
    row_mats = []
    for v in range(2):
        mr, mi = row_rot * e2r[v : v + 1, :], row_rot * e2i[v : v + 1, :]
        row_mats.append(
            split(
                jnp.concatenate(
                    [jnp.concatenate([mr, -mi], axis=1), jnp.concatenate([mi, mr], axis=1)], axis=0
                )
            )
        )

    def lanes_done(rl):
        xre = x_ref[pl.ds(2 * rl, 128, stride=32), :]
        xim = x_ref[pl.ds(2 * rl + 1, 128, stride=32), :]
        er, ei = e1r[rl : rl + 1, :], e1i[rl : rl + 1, :]
        y = jnp.concatenate([xre * er - xim * ei, xre * ei + xim * er], axis=0)
        y_hi, y_lo = split(y)
        p = jnp.dot(jnp.concatenate([y_hi, y_lo], axis=1), lane_mat, preferred_element_type=F32)
        return p[:, :128] + p[:, 128:]

    for rl in range(0, 16, 2):
        m_hi, m_lo = row_mats[rl >> 3]
        y_hi, y_lo = split(jnp.concatenate([lanes_done(rl), lanes_done(rl + 1)], axis=1))
        z = jnp.dot(m_hi, y_hi, preferred_element_type=F32)
        z = z + jnp.dot(m_lo, y_hi, preferred_element_type=F32)
        z = z + jnp.dot(m_hi, y_lo, preferred_element_type=F32)
        z_ref[rl] = z[:, :128]
        z_ref[rl + 1] = z[:, 128:]

    low_tangents = [jnp.broadcast_to(tangents[7 + k : 8 + k, :], (8, 128)) for k in range(4)]
    for at in range(0, 256, 8):
        v = [z_ref[rl, at : at + 8, :] for rl in range(16)]
        for k in range(4):
            t = low_tangents[k]
            w = list(v)
            for rl in range(16):
                if rl >> k & 1:
                    w[rl] = v[rl] + t * v[rl ^ (1 << k)]
                else:
                    w[rl] = v[rl] - t * v[rl ^ (1 << k)]
            v = w
        for rl in range(16):
            row = rl * 256 + at
            s = max(i for i in range(len(SIZES)) if STARTS[i] <= row)
            outs[s][row - STARTS[s] : row - STARTS[s] + 8, :] = v[rl]


def final_kernel(*refs):
    ins, out_ref = refs[: len(SIZES)], refs[len(SIZES)]
    number = device_bits()
    device_ones = number & 1
    for k in range(1, 7):
        device_ones = device_ones + ((number >> k) & 1)
    rows = lax.broadcasted_iota(jnp.int32, (128, 128), 0)
    cols = lax.broadcasted_iota(jnp.int32, (128, 128), 1)
    base = ones_in(rows, 7) + ones_in(cols, 7) + device_ones

    def read(start):
        parts = []
        row = start
        while row < start + 128:
            s = max(i for i in range(len(SIZES)) if STARTS[i] <= row)
            stop = min(start + 128, STARTS[s] + SIZES[s])
            parts.append(ins[s][row - STARTS[s] : stop - STARTS[s], :])
            row = stop
        return parts[0] if len(parts) == 1 else jnp.concatenate(parts, axis=0)

    for rl in range(16):
        re, im = read(rl * 256), read(rl * 256 + 128)
        quarter = (base + bin(rl).count("1")) & 3
        odd = (quarter & 1) == 1
        out_re = jnp.where(odd, im, re)
        out_im = jnp.where(odd, re, im)
        out_ref[pl.ds(2 * rl, 128, stride=32), :] = jnp.where(quarter >= 2, -out_re, out_re)
        out_ref[pl.ds(2 * rl + 1, 128, stride=32), :] = jnp.where(
            (quarter == 1) | (quarter == 2), -out_im, out_im
        )


def exchange_order():
    count = len(SIZES)
    return [(i, step) for step in ("c", 0, 1, 2, 3, 4, 5) for i in range(count)]


def shards(amplitudes, couplings, fields):
    rows = amplitudes.reshape(2, 2048, 128).transpose(1, 0, 2).reshape(4096, 128)
    vmem = pl.BlockSpec(memory_space=pltpu.VMEM)
    smem = pl.BlockSpec(memory_space=pltpu.SMEM)
    made = pl.pallas_call(
        local_kernel,
        out_shape=[pltpu.VMEM((s, 128), F32) for s in SIZES] + [pltpu.VMEM((16, 128), F32)],
        in_specs=[vmem, smem, smem],
        out_specs=[vmem] * (len(SIZES) + 1),
        scratch_shapes=[pltpu.VMEM((16, 256, 128), F32)],
        name="local_step",
    )(rows, couplings, fields)
    streams, coef = list(made[:-1]), made[-1]

    count = len(streams)
    kept = [None] * count
    for i, step in exchange_order():
        if step == "c":
            got = lax.ppermute(streams[i], AXES, pairs_of("c", True))
            streams[i] = streams[i] + coef[9:10] * got
            continue
        first = step % 2 == 0
        k = (step // 2 + i) % 3
        got = lax.ppermute(streams[i], AXES, pairs_of("xyz"[k], first))
        if first:
            mine = streams[i]
            kept[i] = mine + coef[3 * k : 3 * k + 1] * got
            streams[i] = coef[3 * k + 1 : 3 * k + 2] * mine + coef[3 * k + 2 : 3 * k + 3] * got
        else:
            streams[i] = kept[i] + got
    out = pl.pallas_call(
        final_kernel,
        out_shape=jax.ShapeDtypeStruct((4096, 128), F32),
        in_specs=[vmem] * count,
        out_specs=vmem,
        name="final_step",
    )(*[pltpu.with_memory_space_constraint(s, pltpu.VMEM) for s in streams])
    return out.reshape(2048, 2, 128).transpose(1, 0, 2).reshape(2, 262144)


def solution(mesh):
    placed = (P(None, AXES), P(), P())
    return jax.shard_map(shards, mesh=mesh, in_specs=placed, out_specs=P(None, AXES), check_vma=False)
```

```python
import jax
import jax.numpy as jnp
from jax import lax
from jax.experimental import pallas as pl
from jax.experimental.pallas import tpu as pltpu
from jax.sharding import PartitionSpec as P


AXES = ("gx", "gy", "gz")
SHAPES = ((688, 128), (680, 128), (85, 8, 128), (43, 16, 128), (5, 136, 128), (17, 40, 128))
ROWS = (688, 680, 680, 688, 680, 680)
FIRST_DIM = (0, 1, 2, 0, 1, 2)
COUNT = len(SHAPES)
HALF = COUNT // 2
BASES = tuple(sum(ROWS[:i]) for i in range(COUNT))
F32 = jnp.float32
BF16 = jnp.bfloat16


def pair_table():
    place, table = {}, {}
    for gx in range(8):
        for gy in range(2):
            for gz in range(8):
                place[(gx >> 1, gx & 1, (gz & 1) * 2 + gy, gz >> 1)] = (gx * 2 + gy) * 8 + gz
    for (z, core, x, y), device in place.items():
        table[device] = {
            "core": core,
            "c": place[(z, core ^ 1, x, y)],
            "xA": place[(z, core, x ^ 1, y)],
            "xB": place[(z, core, x ^ 3, y)],
            "yA": place[(z, core, x, y ^ 1)],
            "yB": place[(z, core, x, y ^ 3)],
            "zA": place[(z ^ 1, core, x, y)],
            "zB": place[(z ^ 3, core, x, y)],
        }
    return table


def pairs_of(dim, first):
    table = pair_table()
    if dim == "c":
        return [(d, row["c"]) for d, row in table.items()]
    return [(d, row[dim + ("A" if (row["core"] == 0) == first else "B")]) for d, row in table.items()]


def spin(value, bit):
    return 1.0 - 2.0 * ((value >> bit) & 1).astype(F32)


def ones_in(value, bits):
    total = value & 1
    for bit in range(1, bits):
        total = total + ((value >> bit) & 1)
    return total


def turn(cosine, sine, quarter):
    quarter = quarter & 3
    odd = (quarter & 1) == 1
    real = jnp.where(odd, sine, cosine)
    imag = jnp.where(odd, cosine, -sine)
    sign = jnp.where(quarter >= 2, -1.0, 1.0)
    return real * sign, imag * sign


def split(value):
    high = value.astype(BF16)
    return high, (value - high.astype(F32)).astype(BF16)


def rotation(tangents, first, right):
    rows = lax.broadcasted_iota(jnp.int32, (128, 128), 0)
    cols = lax.broadcasted_iota(jnp.int32, (128, 128), 1)
    out_at, in_at = (cols, rows) if right else (rows, cols)
    differ = out_at ^ in_at
    result = jnp.ones((128, 128), F32)
    for bit in range(7):
        tangent = tangents[first + bit : first + bit + 1, :]
        signed = jnp.where(((out_at >> bit) & 1) == 1, tangent, -tangent)
        result = result * jnp.where(((differ >> bit) & 1) == 1, signed, 1.0)
    return result


def device_bits():
    number = (lax.axis_index("gx") * 2 + lax.axis_index("gy")) * 8 + lax.axis_index("gz")
    return number


def window(refs, base, row, rows):
    s = max(i for i in range(base, base + len(refs)) if BASES[i] <= row)
    at = row - BASES[s]
    if len(SHAPES[s]) == 2:
        return refs[s - base], (slice(at, at + rows), slice(None))
    per = SHAPES[s][1]
    return refs[s - base], (at // per, slice(at % per, at % per + rows), slice(None))


def phase_kernel(x_hbm, j_ref, f_ref, *refs):
    outs, (coef_ref, lane_ref, high_ref, x_ref, sems) = refs[:COUNT], refs[COUNT:]
    copies = [
        pltpu.make_async_copy(x_hbm.at[pl.ds(1024 * h, 1024), :], x_ref.at[pl.ds(1024 * h, 1024), :], sems.at[h])
        for h in range(4)
    ]
    for copy in copies:
        copy.start()
    number = device_bits()
    bits = [(number >> k) & 1 for k in range(7)]
    sigma = [1.0 - 2.0 * b.astype(F32) for b in bits]
    row_at = lax.broadcasted_iota(jnp.int32, (32, 128), 0)
    angles = jnp.zeros((32, 128), F32)
    for q in range(25):
        angles = jnp.where(row_at == q, f_ref[q], angles)
    cosines = jnp.cos(angles)
    tangents = jnp.sin(angles) / cosines
    scale = cosines[0:1, :]
    for q in range(1, 25):
        scale = scale * cosines[q : q + 1, :]

    on_core0 = bits[4] == 0
    table = jnp.zeros((16, 128), F32)
    row16 = lax.broadcasted_iota(jnp.int32, (16, 128), 0)

    def put(table, row, value):
        return jnp.where(row16 == row, value, table)

    for k, (q0, q1) in enumerate(((21, 18), (19, 20), (23, 24))):
        s0 = -sigma[q0 - 18] * tangents[q0 : q0 + 1, :]
        s1 = -sigma[q1 - 18] * tangents[q1 : q1 + 1, :]
        both = s0 * s1
        table = put(table, 3 * k, jnp.where(on_core0, s0, both))
        table = put(table, 3 * k + 1, jnp.where(on_core0, both, -s0))
        table = put(table, 3 * k + 2, jnp.where(on_core0, -s1, s1))
    table = put(table, 9, -sigma[4] * tangents[22:23, :])
    coef_ref[...] = table

    low = lax.broadcasted_iota(jnp.int32, (16, 128), 0) * 128 + lax.broadcasted_iota(jnp.int32, (16, 128), 1)
    spins = [spin(low, q) for q in range(11)]
    phase = j_ref[24] * sigma[6] * spins[0]
    for q in range(10):
        phase = phase + j_ref[q] * (spins[q] * spins[q + 1])
    e1r, e1i = turn(jnp.cos(phase), jnp.sin(phase), ones_in(low, 11))
    high = lax.broadcasted_iota(jnp.int32, (8, 128), 1)
    spins = [spin(high, k) for k in range(7)]
    below = spin(lax.broadcasted_iota(jnp.int32, (8, 128), 0), 0)
    phase = j_ref[10] * (below * spins[0]) + (j_ref[17] * sigma[0]) * spins[6]
    for k in range(6):
        phase = phase + j_ref[11 + k] * (spins[k] * spins[k + 1])
    of_device = j_ref[18] * (sigma[0] * sigma[1])
    for k in range(1, 6):
        of_device = of_device + j_ref[18 + k] * (sigma[k] * sigma[k + 1])
    phase = phase + of_device
    device_ones = bits[0] + bits[1] + bits[2] + bits[3] + bits[4] + bits[5] + bits[6]
    e2r, e2i = turn(jnp.cos(phase), jnp.sin(phase), ones_in(high, 7) + device_ones)
    e2r, e2i = e2r * scale, e2i * scale
    columns = [
        [jnp.transpose(jnp.broadcast_to(e[v : v + 1, :], (128, 128))) for e in (e2r, e2i)] for v in range(2)
    ]

    lane_hi, lane_lo = split(rotation(tangents, 0, True))
    lane_ref[0:128, 0:128] = lane_hi
    lane_ref[0:128, 128:256] = lane_lo
    lane_ref[128:256, 0:128] = lane_hi
    lane_ref[128:256, 128:256] = jnp.zeros((128, 128), BF16)
    high_hi, high_lo = split(rotation(tangents, 11, False))
    high_ref[:, 0:128] = high_hi
    high_ref[:, 128:256] = high_lo
    high_ref[:, 256:384] = high_hi

    low_tangents = [jnp.broadcast_to(tangents[7 + k : 8 + k, :], (8, 128)) for k in range(4)]
    for at in range(0, 128, 8):
        if at % 32 == 0:
            copies[at // 32].wait()
        values = [[], []]
        for rl in range(16):
            xre = x_ref[pl.ds(at * 32 + 2 * rl, 8, stride=32), :]
            xim = x_ref[pl.ds(at * 32 + 2 * rl + 1, 8, stride=32), :]
            er, ei = e1r[rl : rl + 1, :], e1i[rl : rl + 1, :]
            cr, ci = (c[at : at + 8, :] for c in columns[rl >> 3])
            yre, yim = xre * er - xim * ei, xre * ei + xim * er
            values[0].append(yre * cr - yim * ci)
            values[1].append(yre * ci + yim * cr)
        for c in range(2):
            v = values[c]
            for k in range(4):
                t = low_tangents[k]
                v = [
                    v[rl] + t * v[rl ^ (1 << k)] if rl >> k & 1 else v[rl] - t * v[rl ^ (1 << k)]
                    for rl in range(16)
                ]
            for rl in range(16):
                ref, index = window(outs, 0, (2 * rl + c) * 128 + at, 8)
                ref[index] = v[rl]


def finish(ins, base, lane_ref, high_ref, out_hbm, o_ref, sems):
    number = device_bits()
    device_ones = number & 1
    for k in range(1, 7):
        device_ones = device_ones + ((number >> k) & 1)
    rows = lax.broadcasted_iota(jnp.int32, (128, 128), 0)
    cols = lax.broadcasted_iota(jnp.int32, (128, 128), 1)
    turns = ones_in(rows, 7) + ones_in(cols, 7) + device_ones
    first = 0 if base == 0 else 8

    def read(row):
        parts = []
        for at in range(row, row + 128, 8):
            ref, index = window(ins, base, at, 8)
            parts.append(ref[index])
        return jnp.concatenate(parts, axis=0)

    copies = []
    for rl in range(first, first + 8):
        y = jnp.concatenate([read(rl * 256), read(rl * 256 + 128)], axis=0)
        y_hi, y_lo = split(y)
        p = jnp.dot(jnp.concatenate([y_hi, y_lo], axis=1), lane_ref[...], preferred_element_type=F32)
        y = p[:, :128] + p[:, 128:]
        y_hi, y_lo = split(jnp.concatenate([y[:128], y[128:]], axis=1))
        z = jnp.dot(high_ref[...], jnp.concatenate([y_hi, y_hi, y_lo], axis=0), preferred_element_type=F32)
        re, im = z[:, :128], z[:, 128:]
        quarter = (turns + bin(rl).count("1")) & 3
        odd = (quarter & 1) == 1
        out_re = jnp.where(odd, im, re)
        out_im = jnp.where(odd, re, im)
        at = 2 * (rl - first)
        o_ref[pl.ds(at, 128, stride=16), :] = jnp.where(quarter >= 2, -out_re, out_re)
        o_ref[pl.ds(at + 1, 128, stride=16), :] = jnp.where((quarter == 1) | (quarter == 2), -out_im, out_im)
        if rl % 4 == 3:
            part = (rl - first) // 4
            copies.append(
                pltpu.make_async_copy(
                    o_ref.reshape(128, 16, 128).at[:, pl.ds(8 * part, 8), :],
                    out_hbm.at[:, pl.ds(2 * first + 8 * part, 8), :],
                    sems.at[part],
                )
            )
            copies[-1].start()
    for copy in copies:
        copy.wait()


def first_final_kernel(*refs):
    finish(refs[:HALF], 0, *refs[HALF:])


def second_final_kernel(*refs):
    finish(refs[:HALF], HALF, refs[HALF], refs[HALF + 1], *refs[HALF + 3 :])


def exchange_order():
    return [(i, step) for step in ("c", 0, 1, 2, 3, 4, 5) for i in range(COUNT)]


def shards(amplitudes, couplings, fields):
    rows = amplitudes.reshape(2, 2048, 128).transpose(1, 0, 2).reshape(4096, 128)
    vmem = pl.BlockSpec(memory_space=pltpu.VMEM)
    smem = pl.BlockSpec(memory_space=pltpu.SMEM)
    hbm = pl.BlockSpec(memory_space=pl.ANY)
    made = pl.pallas_call(
        phase_kernel,
        out_shape=[pltpu.VMEM(s, F32) for s in SHAPES]
        + [pltpu.VMEM((16, 128), F32), pltpu.VMEM((256, 256), BF16), pltpu.VMEM((128, 384), BF16)],
        in_specs=[hbm, smem, smem],
        out_specs=[vmem] * (COUNT + 3),
        scratch_shapes=[pltpu.VMEM((4096, 128), F32), pltpu.SemaphoreType.DMA((4,))],
        name="phase_step",
    )(rows, couplings, fields)
    streams, (coef, lane_mat, high_mat) = list(made[:COUNT]), made[COUNT:]

    kept = [None] * COUNT
    for i, step in exchange_order():
        if step == "c":
            got = lax.ppermute(streams[i], AXES, pairs_of("c", True))
            streams[i] = streams[i] + coef[9:10] * got
            continue
        first = step % 2 == 0
        k = (step // 2 + FIRST_DIM[i]) % 3
        got = lax.ppermute(streams[i], AXES, pairs_of("xyz"[k], first))
        if first:
            mine = streams[i]
            kept[i] = mine + coef[3 * k : 3 * k + 1] * got
            streams[i] = coef[3 * k + 1 : 3 * k + 2] * mine + coef[3 * k + 2 : 3 * k + 3] * got
        else:
            streams[i] = kept[i] + got

    def held(value):
        return pltpu.with_memory_space_constraint(value, pltpu.VMEM)

    scratch = [pltpu.VMEM((2048, 128), F32), pltpu.SemaphoreType.DMA((2,))]
    out_shape = jax.ShapeDtypeStruct((128, 32, 128), F32)
    out = pl.pallas_call(
        first_final_kernel,
        out_shape=out_shape,
        in_specs=[vmem] * (HALF + 2),
        out_specs=hbm,
        scratch_shapes=scratch,
        compiler_params=pltpu.CompilerParams(vmem_limit_bytes=8 << 20),
        name="first_final",
    )(*[held(v) for v in streams[:HALF]], held(lane_mat), held(high_mat))
    out = pl.pallas_call(
        second_final_kernel,
        out_shape=out_shape,
        in_specs=[vmem] * (HALF + 2) + [hbm],
        out_specs=hbm,
        scratch_shapes=scratch,
        input_output_aliases={HALF + 2: 0},
        compiler_params=pltpu.CompilerParams(vmem_limit_bytes=8 << 20),
        name="second_final",
    )(*[held(v) for v in streams[HALF:]], held(lane_mat), held(high_mat), out)
    return out.reshape(2048, 2, 128).transpose(1, 0, 2).reshape(2, 262144)


def solution(mesh):
    placed = (P(None, AXES), P(), P())
    return jax.shard_map(shards, mesh=mesh, in_specs=placed, out_specs=P(None, AXES), check_vma=False)
```

```python
import jax
import jax.numpy as jnp
from jax import lax
from jax.experimental import pallas as pl
from jax.experimental.pallas import tpu as pltpu
from jax.sharding import PartitionSpec as P


AXES = ("gx", "gy", "gz")
SHAPES = ((688, 128), (680, 128), (85, 8, 128), (43, 16, 128), (5, 136, 128), (17, 40, 128))
ROWS = (688, 680, 680, 688, 680, 680)
FIRST_DIM = (0, 1, 2, 1, 2, 0)
COUNT = len(SHAPES)
HALF = COUNT // 2
BASES = tuple(sum(ROWS[:i]) for i in range(COUNT))
F32 = jnp.float32
BF16 = jnp.bfloat16


def pair_table():
    place, table = {}, {}
    for gx in range(8):
        for gy in range(2):
            for gz in range(8):
                place[(gx >> 1, gx & 1, (gz & 1) * 2 + gy, gz >> 1)] = (gx * 2 + gy) * 8 + gz
    for (z, core, x, y), device in place.items():
        table[device] = {
            "core": core,
            "c": place[(z, core ^ 1, x, y)],
            "xA": place[(z, core, x ^ 1, y)],
            "xB": place[(z, core, x ^ 3, y)],
            "yA": place[(z, core, x, y ^ 1)],
            "yB": place[(z, core, x, y ^ 3)],
            "zA": place[(z ^ 1, core, x, y)],
            "zB": place[(z ^ 3, core, x, y)],
        }
    return table


def pairs_of(dim, first):
    table = pair_table()
    if dim == "c":
        return [(d, row["c"]) for d, row in table.items()]
    return [(d, row[dim + ("A" if (row["core"] == 0) == first else "B")]) for d, row in table.items()]


def spin(value, bit):
    return 1.0 - 2.0 * ((value >> bit) & 1).astype(F32)


def ones_in(value, bits):
    total = value & 1
    for bit in range(1, bits):
        total = total + ((value >> bit) & 1)
    return total


def turn(cosine, sine, quarter):
    quarter = quarter & 3
    odd = (quarter & 1) == 1
    real = jnp.where(odd, sine, cosine)
    imag = jnp.where(odd, cosine, -sine)
    sign = jnp.where(quarter >= 2, -1.0, 1.0)
    return real * sign, imag * sign


def split(value):
    high = value.astype(BF16)
    return high, (value - high.astype(F32)).astype(BF16)


def rotation(tangents, first, right):
    rows = lax.broadcasted_iota(jnp.int32, (128, 128), 0)
    cols = lax.broadcasted_iota(jnp.int32, (128, 128), 1)
    out_at, in_at = (cols, rows) if right else (rows, cols)
    differ = out_at ^ in_at
    result = jnp.ones((128, 128), F32)
    for bit in range(7):
        tangent = tangents[first + bit : first + bit + 1, :]
        signed = jnp.where(((out_at >> bit) & 1) == 1, tangent, -tangent)
        result = result * jnp.where(((differ >> bit) & 1) == 1, signed, 1.0)
    return result


def device_bits():
    number = (lax.axis_index("gx") * 2 + lax.axis_index("gy")) * 8 + lax.axis_index("gz")
    return number


def window(refs, base, row, rows):
    s = max(i for i in range(base, base + len(refs)) if BASES[i] <= row)
    at = row - BASES[s]
    if len(SHAPES[s]) == 2:
        return refs[s - base], (slice(at, at + rows), slice(None))
    per = SHAPES[s][1]
    return refs[s - base], (at // per, slice(at % per, at % per + rows), slice(None))


def phase_kernel(x_hbm, j_ref, f_ref, *refs):
    outs, (coef_ref, tan_ref, x_ref, sems) = refs[:COUNT], refs[COUNT:]
    copies = [
        pltpu.make_async_copy(x_hbm.at[pl.ds(1024 * h, 1024), :], x_ref.at[pl.ds(1024 * h, 1024), :], sems.at[h])
        for h in range(4)
    ]
    for copy in copies:
        copy.start()
    number = device_bits()
    bits = [(number >> k) & 1 for k in range(7)]
    sigma = [1.0 - 2.0 * b.astype(F32) for b in bits]
    row_at = lax.broadcasted_iota(jnp.int32, (32, 128), 0)
    angles = jnp.zeros((32, 128), F32)
    for q in range(25):
        angles = jnp.where(row_at == q, f_ref[q], angles)
    cosines = jnp.cos(angles)
    tangents = jnp.sin(angles) / cosines
    scale = cosines[0:1, :]
    for q in range(1, 25):
        scale = scale * cosines[q : q + 1, :]

    on_core0 = bits[4] == 0
    table = jnp.zeros((16, 128), F32)
    row16 = lax.broadcasted_iota(jnp.int32, (16, 128), 0)

    def put(table, row, value):
        return jnp.where(row16 == row, value, table)

    for k, (q0, q1) in enumerate(((21, 18), (19, 20), (23, 24))):
        s0 = -sigma[q0 - 18] * tangents[q0 : q0 + 1, :]
        s1 = -sigma[q1 - 18] * tangents[q1 : q1 + 1, :]
        both = s0 * s1
        table = put(table, 3 * k, jnp.where(on_core0, s0, both))
        table = put(table, 3 * k + 1, jnp.where(on_core0, both, -s0))
        table = put(table, 3 * k + 2, jnp.where(on_core0, -s1, s1))
    table = put(table, 9, -sigma[4] * tangents[22:23, :])
    coef_ref[...] = table

    low = lax.broadcasted_iota(jnp.int32, (16, 128), 0) * 128 + lax.broadcasted_iota(jnp.int32, (16, 128), 1)
    spins = [spin(low, q) for q in range(11)]
    phase = j_ref[24] * sigma[6] * spins[0]
    for q in range(10):
        phase = phase + j_ref[q] * (spins[q] * spins[q + 1])
    e1r, e1i = turn(jnp.cos(phase), jnp.sin(phase), ones_in(low, 11))
    high = lax.broadcasted_iota(jnp.int32, (8, 128), 1)
    spins = [spin(high, k) for k in range(7)]
    below = spin(lax.broadcasted_iota(jnp.int32, (8, 128), 0), 0)
    phase = j_ref[10] * (below * spins[0]) + (j_ref[17] * sigma[0]) * spins[6]
    for k in range(6):
        phase = phase + j_ref[11 + k] * (spins[k] * spins[k + 1])
    of_device = j_ref[18] * (sigma[0] * sigma[1])
    for k in range(1, 6):
        of_device = of_device + j_ref[18 + k] * (sigma[k] * sigma[k + 1])
    phase = phase + of_device
    device_ones = bits[0] + bits[1] + bits[2] + bits[3] + bits[4] + bits[5] + bits[6]
    e2r, e2i = turn(jnp.cos(phase), jnp.sin(phase), ones_in(high, 7) + device_ones)
    e2r, e2i = e2r * scale, e2i * scale
    columns = [
        [jnp.transpose(jnp.broadcast_to(e[v : v + 1, :], (128, 128))) for e in (e2r, e2i)] for v in range(2)
    ]

    tan_ref[...] = tangents

    low_tangents = [jnp.broadcast_to(tangents[7 + k : 8 + k, :], (8, 128)) for k in range(4)]
    for at in range(0, 128, 8):
        if at % 32 == 0:
            copies[at // 32].wait()
        values = [[], []]
        for rl in range(16):
            xre = x_ref[pl.ds(at * 32 + 2 * rl, 8, stride=32), :]
            xim = x_ref[pl.ds(at * 32 + 2 * rl + 1, 8, stride=32), :]
            er, ei = e1r[rl : rl + 1, :], e1i[rl : rl + 1, :]
            cr, ci = (c[at : at + 8, :] for c in columns[rl >> 3])
            yre, yim = xre * er - xim * ei, xre * ei + xim * er
            values[0].append(yre * cr - yim * ci)
            values[1].append(yre * ci + yim * cr)
        for c in range(2):
            v = values[c]
            for k in range(4):
                t = low_tangents[k]
                v = [
                    v[rl] + t * v[rl ^ (1 << k)] if rl >> k & 1 else v[rl] - t * v[rl ^ (1 << k)]
                    for rl in range(16)
                ]
            for rl in range(16):
                ref, index = window(outs, 0, (2 * rl + c) * 128 + at, 8)
                ref[index] = v[rl]


def finish(ins, base, first, last, lane_ref, high_ref, out_hbm, o_ref, sems):
    number = device_bits()
    device_ones = number & 1
    for k in range(1, 7):
        device_ones = device_ones + ((number >> k) & 1)
    rows = lax.broadcasted_iota(jnp.int32, (128, 128), 0)
    cols = lax.broadcasted_iota(jnp.int32, (128, 128), 1)
    turns = ones_in(rows, 7) + ones_in(cols, 7) + device_ones
    width = 2 * (last - first)

    def read(row):
        parts = []
        for at in range(row, row + 128, 8):
            ref, index = window(ins, base, at, 8)
            parts.append(ref[index])
        return jnp.concatenate(parts, axis=0)

    copies = []
    for rl in range(first, last):
        y = jnp.concatenate([read(rl * 256), read(rl * 256 + 128)], axis=0)
        y_hi, y_lo = split(y)
        p = jnp.dot(jnp.concatenate([y_hi, y_lo], axis=1), lane_ref[...], preferred_element_type=F32)
        y = p[:, :128] + p[:, 128:]
        y_hi, y_lo = split(jnp.concatenate([y[:128], y[128:]], axis=1))
        z = jnp.dot(high_ref[...], jnp.concatenate([y_hi, y_hi, y_lo], axis=0), preferred_element_type=F32)
        re, im = z[:, :128], z[:, 128:]
        quarter = (turns + bin(rl).count("1")) & 3
        odd = (quarter & 1) == 1
        out_re = jnp.where(odd, im, re)
        out_im = jnp.where(odd, re, im)
        at = 2 * (rl - first)
        o_ref[pl.ds(at, 128, stride=width), :] = jnp.where(quarter >= 2, -out_re, out_re)
        o_ref[pl.ds(at + 1, 128, stride=width), :] = jnp.where((quarter == 1) | (quarter == 2), -out_im, out_im)
        if rl % 4 == 3:
            part = (rl - first) // 4
            copies.append(
                pltpu.make_async_copy(
                    o_ref.reshape(128, width, 128).at[:, pl.ds(8 * part, 8), :],
                    out_hbm.at[:, pl.ds(2 * first + 8 * part, 8), :],
                    sems.at[part],
                )
            )
            copies[-1].start()
    for copy in copies:
        copy.wait()


def first_final_kernel(*refs):
    ins, (tan_ref, out_hbm, lane_ref, high_ref, o_ref, sems) = refs[:HALF], refs[HALF:]
    tangents = tan_ref[...]
    lane_hi, lane_lo = split(rotation(tangents, 0, True))
    lane_ref[0:128, 0:128] = lane_hi
    lane_ref[0:128, 128:256] = lane_lo
    lane_ref[128:256, 0:128] = lane_hi
    lane_ref[128:256, 128:256] = jnp.zeros((128, 128), BF16)
    high_hi, high_lo = split(rotation(tangents, 11, False))
    high_ref[:, 0:128] = high_hi
    high_ref[:, 128:256] = high_lo
    high_ref[:, 256:384] = high_hi
    finish(ins, 0, 0, 8, lane_ref, high_ref, out_hbm, o_ref, sems)


def second_final_kernel(*refs):
    finish(refs[:HALF], HALF, 8, 16, refs[HALF], refs[HALF + 1], *refs[HALF + 3 :])


def exchange_order():
    return [(i, step) for step in ("c", 0, 1, 2, 3, 4, 5) for i in range(COUNT)]


def shards(amplitudes, couplings, fields):
    rows = amplitudes.reshape(2, 2048, 128).transpose(1, 0, 2).reshape(4096, 128)
    vmem = pl.BlockSpec(memory_space=pltpu.VMEM)
    smem = pl.BlockSpec(memory_space=pltpu.SMEM)
    hbm = pl.BlockSpec(memory_space=pl.ANY)
    made = pl.pallas_call(
        phase_kernel,
        out_shape=[pltpu.VMEM(s, F32) for s in SHAPES]
        + [pltpu.VMEM((16, 128), F32), pltpu.VMEM((32, 128), F32)],
        in_specs=[hbm, smem, smem],
        out_specs=[vmem] * (COUNT + 2),
        scratch_shapes=[pltpu.VMEM((4096, 128), F32), pltpu.SemaphoreType.DMA((4,))],
        name="phase_step",
    )(rows, couplings, fields)
    streams, (coef, tangents) = list(made[:COUNT]), made[COUNT:]

    kept = [None] * COUNT
    for i, step in exchange_order():
        if step == "c":
            got = lax.ppermute(streams[i], AXES, pairs_of("c", True))
            streams[i] = streams[i] + coef[9:10] * got
            continue
        first = step % 2 == 0
        k = (step // 2 + FIRST_DIM[i]) % 3
        got = lax.ppermute(streams[i], AXES, pairs_of("xyz"[k], first))
        if first:
            mine = streams[i]
            kept[i] = mine + coef[3 * k : 3 * k + 1] * got
            streams[i] = coef[3 * k + 1 : 3 * k + 2] * mine + coef[3 * k + 2 : 3 * k + 3] * got
        else:
            streams[i] = kept[i] + got

    def held(value):
        return pltpu.with_memory_space_constraint(value, pltpu.VMEM)

    out_shape = jax.ShapeDtypeStruct((128, 32, 128), F32)
    scratch = [pltpu.VMEM((2048, 128), F32), pltpu.SemaphoreType.DMA((2,))]
    params = pltpu.CompilerParams(vmem_limit_bytes=8 << 20)
    out, lane_mat, high_mat = pl.pallas_call(
        first_final_kernel,
        out_shape=[out_shape, pltpu.VMEM((256, 256), BF16), pltpu.VMEM((128, 384), BF16)],
        in_specs=[vmem] * (HALF + 1),
        out_specs=[hbm, vmem, vmem],
        scratch_shapes=scratch,
        compiler_params=params,
        name="first_final",
    )(*[held(v) for v in streams[:HALF]], held(tangents))
    out = pl.pallas_call(
        second_final_kernel,
        out_shape=out_shape,
        in_specs=[vmem] * (HALF + 2) + [hbm],
        out_specs=hbm,
        scratch_shapes=scratch,
        compiler_params=params,
        input_output_aliases={HALF + 2: 0},
        name="second_final",
    )(*[held(v) for v in streams[HALF:]], held(lane_mat), held(high_mat), out)
    return out.reshape(2048, 2, 128).transpose(1, 0, 2).reshape(2, 262144)


def solution(mesh):
    placed = (P(None, AXES), P(), P())
    return jax.shard_map(shards, mesh=mesh, in_specs=placed, out_specs=P(None, AXES), check_vma=False)
```

```python
import jax
import jax.numpy as jnp
from jax import lax
from jax.experimental import pallas as pl
from jax.experimental.pallas import tpu as pltpu
from jax.sharding import PartitionSpec as P


AXES = ("gx", "gy", "gz")
SHAPES = ((688, 128), (680, 128), (85, 8, 128), (43, 16, 128), (5, 136, 128), (17, 40, 128))
ROWS = (688, 680, 680, 688, 680, 680)
FIRST_DIM = (0, 1, 2, 1, 2, 0)
COUNT = len(SHAPES)
HALF = COUNT // 2
BASES = tuple(sum(ROWS[:i]) for i in range(COUNT))
F32 = jnp.float32
BF16 = jnp.bfloat16


def pair_table():
    place, table = {}, {}
    for gx in range(8):
        for gy in range(2):
            for gz in range(8):
                place[(gx >> 1, gx & 1, (gz & 1) * 2 + gy, gz >> 1)] = (gx * 2 + gy) * 8 + gz
    for (z, core, x, y), device in place.items():
        table[device] = {
            "core": core,
            "c": place[(z, core ^ 1, x, y)],
            "xA": place[(z, core, x ^ 1, y)],
            "xB": place[(z, core, x ^ 3, y)],
            "yA": place[(z, core, x, y ^ 1)],
            "yB": place[(z, core, x, y ^ 3)],
            "zA": place[(z ^ 1, core, x, y)],
            "zB": place[(z ^ 3, core, x, y)],
        }
    return table


def pairs_of(dim, first):
    table = pair_table()
    if dim == "c":
        return [(d, row["c"]) for d, row in table.items()]
    return [(d, row[dim + ("A" if (row["core"] == 0) == first else "B")]) for d, row in table.items()]


def spin(value, bit):
    return 1.0 - 2.0 * ((value >> bit) & 1).astype(F32)


def ones_in(value, bits):
    total = value & 1
    for bit in range(1, bits):
        total = total + ((value >> bit) & 1)
    return total


def turn(cosine, sine, quarter):
    quarter = quarter & 3
    odd = (quarter & 1) == 1
    real = jnp.where(odd, sine, cosine)
    imag = jnp.where(odd, cosine, -sine)
    sign = jnp.where(quarter >= 2, -1.0, 1.0)
    return real * sign, imag * sign


def split(value):
    high = value.astype(BF16)
    return high, (value - high.astype(F32)).astype(BF16)


def rotation(tangents, first, right):
    rows = lax.broadcasted_iota(jnp.int32, (128, 128), 0)
    cols = lax.broadcasted_iota(jnp.int32, (128, 128), 1)
    out_at, in_at = (cols, rows) if right else (rows, cols)
    differ = out_at ^ in_at
    result = jnp.ones((128, 128), F32)
    for bit in range(7):
        tangent = tangents[first + bit : first + bit + 1, :]
        signed = jnp.where(((out_at >> bit) & 1) == 1, tangent, -tangent)
        result = result * jnp.where(((differ >> bit) & 1) == 1, signed, 1.0)
    return result


def device_bits():
    number = (lax.axis_index("gx") * 2 + lax.axis_index("gy")) * 8 + lax.axis_index("gz")
    return number


def window(refs, base, row, rows):
    s = max(i for i in range(base, base + len(refs)) if BASES[i] <= row)
    at = row - BASES[s]
    if len(SHAPES[s]) == 2:
        return refs[s - base], (slice(at, at + rows), slice(None))
    per = SHAPES[s][1]
    return refs[s - base], (at // per, slice(at % per, at % per + rows), slice(None))


def phase_kernel(x_hbm, j_ref, f_ref, *refs):
    outs, (coef_ref, tan_ref, x_ref, sems) = refs[:COUNT], refs[COUNT:]
    copies = [
        pltpu.make_async_copy(
            x_hbm.at[pl.ds(32 * h, 32), :, :],
            x_ref.reshape(128, 40, 128).at[pl.ds(32 * h, 32), pl.ds(0, 32), :],
            sems.at[h],
        )
        for h in range(4)
    ]
    for copy in copies:
        copy.start()
    number = device_bits()
    bits = [(number >> k) & 1 for k in range(7)]
    sigma = [1.0 - 2.0 * b.astype(F32) for b in bits]
    row_at = lax.broadcasted_iota(jnp.int32, (32, 128), 0)
    angles = jnp.zeros((32, 128), F32)
    for q in range(25):
        angles = jnp.where(row_at == q, f_ref[q], angles)
    cosines = jnp.cos(angles)
    tangents = jnp.sin(angles) / cosines
    scale = cosines[0:1, :]
    for q in range(1, 25):
        scale = scale * cosines[q : q + 1, :]

    on_core0 = bits[4] == 0
    table = jnp.zeros((16, 128), F32)
    row16 = lax.broadcasted_iota(jnp.int32, (16, 128), 0)

    def put(table, row, value):
        return jnp.where(row16 == row, value, table)

    for k, (q0, q1) in enumerate(((21, 18), (19, 20), (23, 24))):
        s0 = -sigma[q0 - 18] * tangents[q0 : q0 + 1, :]
        s1 = -sigma[q1 - 18] * tangents[q1 : q1 + 1, :]
        both = s0 * s1
        table = put(table, 3 * k, jnp.where(on_core0, s0, both))
        table = put(table, 3 * k + 1, jnp.where(on_core0, both, -s0))
        table = put(table, 3 * k + 2, jnp.where(on_core0, -s1, s1))
    table = put(table, 9, -sigma[4] * tangents[22:23, :])
    coef_ref[...] = table

    low = lax.broadcasted_iota(jnp.int32, (16, 128), 0) * 128 + lax.broadcasted_iota(jnp.int32, (16, 128), 1)
    spins = [spin(low, q) for q in range(11)]
    phase = j_ref[24] * sigma[6] * spins[0]
    for q in range(10):
        phase = phase + j_ref[q] * (spins[q] * spins[q + 1])
    e1r, e1i = turn(jnp.cos(phase), jnp.sin(phase), ones_in(low, 11))
    high = lax.broadcasted_iota(jnp.int32, (8, 128), 1)
    spins = [spin(high, k) for k in range(7)]
    below = spin(lax.broadcasted_iota(jnp.int32, (8, 128), 0), 0)
    phase = j_ref[10] * (below * spins[0]) + (j_ref[17] * sigma[0]) * spins[6]
    for k in range(6):
        phase = phase + j_ref[11 + k] * (spins[k] * spins[k + 1])
    of_device = j_ref[18] * (sigma[0] * sigma[1])
    for k in range(1, 6):
        of_device = of_device + j_ref[18 + k] * (sigma[k] * sigma[k + 1])
    phase = phase + of_device
    device_ones = bits[0] + bits[1] + bits[2] + bits[3] + bits[4] + bits[5] + bits[6]
    e2r, e2i = turn(jnp.cos(phase), jnp.sin(phase), ones_in(high, 7) + device_ones)
    e2r, e2i = e2r * scale, e2i * scale
    columns = [
        [jnp.transpose(jnp.broadcast_to(e[v : v + 1, :], (128, 128))) for e in (e2r, e2i)] for v in range(2)
    ]

    tan_ref[...] = tangents

    low_tangents = [jnp.broadcast_to(tangents[7 + k : 8 + k, :], (8, 128)) for k in range(4)]
    for at in range(0, 128, 8):
        if at % 32 == 0:
            copies[at // 32].wait()
        values = [[], []]
        for rl in range(16):
            xre = x_ref[pl.ds(at * 40 + 2 * rl, 8, stride=40), :]
            xim = x_ref[pl.ds(at * 40 + 2 * rl + 1, 8, stride=40), :]
            er, ei = e1r[rl : rl + 1, :], e1i[rl : rl + 1, :]
            cr, ci = (c[at : at + 8, :] for c in columns[rl >> 3])
            yre, yim = xre * er - xim * ei, xre * ei + xim * er
            values[0].append(yre * cr - yim * ci)
            values[1].append(yre * ci + yim * cr)
        for c in range(2):
            v = values[c]
            for k in range(4):
                t = low_tangents[k]
                v = [
                    v[rl] + t * v[rl ^ (1 << k)] if rl >> k & 1 else v[rl] - t * v[rl ^ (1 << k)]
                    for rl in range(16)
                ]
            for rl in range(16):
                ref, index = window(outs, 0, (2 * rl + c) * 128 + at, 8)
                ref[index] = v[rl]


def finish(ins, base, first, last, lane_ref, high_ref, out_hbm, o_ref, sems):
    number = device_bits()
    device_ones = number & 1
    for k in range(1, 7):
        device_ones = device_ones + ((number >> k) & 1)
    rows = lax.broadcasted_iota(jnp.int32, (128, 128), 0)
    cols = lax.broadcasted_iota(jnp.int32, (128, 128), 1)
    turns = ones_in(rows, 7) + ones_in(cols, 7) + device_ones
    width = 2 * (last - first) + 8

    def read(row):
        parts = []
        for at in range(row, row + 128, 8):
            ref, index = window(ins, base, at, 8)
            parts.append(ref[index])
        return jnp.concatenate(parts, axis=0)

    copies = []
    for rl in range(first, last):
        y = jnp.concatenate([read(rl * 256), read(rl * 256 + 128)], axis=0)
        y_hi, y_lo = split(y)
        p = jnp.dot(jnp.concatenate([y_hi, y_lo], axis=1), lane_ref[...], preferred_element_type=F32)
        y = p[:, :128] + p[:, 128:]
        y_hi, y_lo = split(jnp.concatenate([y[:128], y[128:]], axis=1))
        z = jnp.dot(high_ref[...], jnp.concatenate([y_hi, y_hi, y_lo], axis=0), preferred_element_type=F32)
        re, im = z[:, :128], z[:, 128:]
        quarter = (turns + bin(rl).count("1")) & 3
        odd = (quarter & 1) == 1
        out_re = jnp.where(odd, im, re)
        out_im = jnp.where(odd, re, im)
        at = 2 * (rl - first)
        o_ref[pl.ds(at, 128, stride=width), :] = jnp.where(quarter >= 2, -out_re, out_re)
        o_ref[pl.ds(at + 1, 128, stride=width), :] = jnp.where((quarter == 1) | (quarter == 2), -out_im, out_im)
        if rl % 4 == 3:
            part = (rl - first) // 4
            copies.append(
                pltpu.make_async_copy(
                    o_ref.reshape(128, width, 128).at[:, pl.ds(8 * part, 8), :],
                    out_hbm.at[:, pl.ds(2 * first + 8 * part, 8), :],
                    sems.at[part],
                )
            )
            copies[-1].start()
    for copy in copies:
        copy.wait()


def first_final_kernel(*refs):
    ins, (tan_ref, out_hbm, lane_ref, high_ref, o_ref, sems) = refs[:HALF], refs[HALF:]
    tangents = tan_ref[...]
    lane_hi, lane_lo = split(rotation(tangents, 0, True))
    lane_ref[0:128, 0:128] = lane_hi
    lane_ref[0:128, 128:256] = lane_lo
    lane_ref[128:256, 0:128] = lane_hi
    lane_ref[128:256, 128:256] = jnp.zeros((128, 128), BF16)
    high_hi, high_lo = split(rotation(tangents, 11, False))
    high_ref[:, 0:128] = high_hi
    high_ref[:, 128:256] = high_lo
    high_ref[:, 256:384] = high_hi
    finish(ins, 0, 0, 8, lane_ref, high_ref, out_hbm, o_ref, sems)


def second_final_kernel(*refs):
    finish(refs[:HALF], HALF, 8, 16, refs[HALF], refs[HALF + 1], *refs[HALF + 3 :])


def exchange_order():
    return [(i, step) for step in ("c", 0, 1, 2, 3, 4, 5) for i in range(COUNT)]


def shards(amplitudes, couplings, fields):
    rows = amplitudes.reshape(2, 2048, 128).transpose(1, 0, 2).reshape(128, 32, 128)
    vmem = pl.BlockSpec(memory_space=pltpu.VMEM)
    smem = pl.BlockSpec(memory_space=pltpu.SMEM)
    hbm = pl.BlockSpec(memory_space=pl.ANY)
    made = pl.pallas_call(
        phase_kernel,
        out_shape=[pltpu.VMEM(s, F32) for s in SHAPES]
        + [pltpu.VMEM((16, 128), F32), pltpu.VMEM((32, 128), F32)],
        in_specs=[hbm, smem, smem],
        out_specs=[vmem] * (COUNT + 2),
        scratch_shapes=[pltpu.VMEM((5120, 128), F32), pltpu.SemaphoreType.DMA((4,))],
        name="phase_step",
    )(rows, couplings, fields)
    streams, (coef, tangents) = list(made[:COUNT]), made[COUNT:]

    kept = [None] * COUNT
    for i, step in exchange_order():
        if step == "c":
            got = lax.ppermute(streams[i], AXES, pairs_of("c", True))
            streams[i] = streams[i] + coef[9:10] * got
            continue
        first = step % 2 == 0
        k = (step // 2 + FIRST_DIM[i]) % 3
        got = lax.ppermute(streams[i], AXES, pairs_of("xyz"[k], first))
        if first:
            mine = streams[i]
            kept[i] = mine + coef[3 * k : 3 * k + 1] * got
            streams[i] = coef[3 * k + 1 : 3 * k + 2] * mine + coef[3 * k + 2 : 3 * k + 3] * got
        else:
            streams[i] = kept[i] + got

    def held(value):
        return pltpu.with_memory_space_constraint(value, pltpu.VMEM)

    out_shape = jax.ShapeDtypeStruct((128, 32, 128), F32)
    scratch = [pltpu.VMEM((3072, 128), F32), pltpu.SemaphoreType.DMA((2,))]
    params = pltpu.CompilerParams(vmem_limit_bytes=8 << 20)
    out, lane_mat, high_mat = pl.pallas_call(
        first_final_kernel,
        out_shape=[out_shape, pltpu.VMEM((256, 256), BF16), pltpu.VMEM((128, 384), BF16)],
        in_specs=[vmem] * (HALF + 1),
        out_specs=[hbm, vmem, vmem],
        scratch_shapes=scratch,
        compiler_params=params,
        name="first_final",
    )(*[held(v) for v in streams[:HALF]], held(tangents))
    out = pl.pallas_call(
        second_final_kernel,
        out_shape=out_shape,
        in_specs=[vmem] * (HALF + 2) + [hbm],
        out_specs=hbm,
        scratch_shapes=scratch,
        compiler_params=params,
        input_output_aliases={HALF + 2: 0},
        name="second_final",
    )(*[held(v) for v in streams[HALF:]], held(lane_mat), held(high_mat), out)
    return out.reshape(2048, 2, 128).transpose(1, 0, 2).reshape(2, 262144)


def solution(mesh):
    placed = (P(None, AXES), P(), P())
    return jax.shard_map(shards, mesh=mesh, in_specs=placed, out_specs=P(None, AXES), check_vma=False)
```
